32 devices in a mesh: north: 8 (over y, x, core), deep: 4 (over z).
Axes of the slice: x: 2, y: 2, z: 4, core: 2. Of those that a mesh axis runs over, the one named last changes fastest.
Arguments:
- velocity: float32 [4, 128, 64, 256], P(None, None, 'north', 'deep'), may hold values from -6 to 6
- coupling: float32 [4, 4], replicated, may hold values from -4 to 4
- symbol_x: float32 [128], replicated, may hold values from 0.3 to 3
- symbol_y: float32 [64], replicated, may hold values from 0.3 to 3
- symbol_z: float32 [256], replicated, may hold values from 0.3 to 3
Outputs:
- spectrum: float32 [4, 128, 64, 256], P(None, 'north', 'deep')
The draws below stay inside these ranges and needn't reach their ends.
All inputs are finite; a program needn't handle non-finite values.
Results may differ from the reference program's by a relative error of at most 0.00007.
Values sent between devices are 32-bit elements; how exact they have to be, the bound alone decides.
A program may use at most 128 MiB of HBM per device.

```python
import jax
import jax.numpy as jnp
from jax import lax

GRID_X = 128
GRID_Y = 64
GRID_Z = 256
FIELDS = 4


def steps_of(rng, dims, pieces, least, top_value):
    loudness = 1.0
    for position, shards_of in pieces:
        steps = jax.random.uniform(jax.random.fold_in(jax.random.fold_in(rng, 6), position), (shards_of,), jnp.float32, least / len(pieces), top_value / len(pieces))
        loudness = loudness * jnp.repeat(jnp.exp(steps), dims[position] // shards_of).reshape((-1,) + (1,) * (len(dims) - 1 - position))
    return loudness


def normal_values(key, shape, deviation, limit, pieces=(), kind=jnp.bfloat16):
    array = jax.random.normal(key, shape, jnp.float32) * deviation
    if len(pieces) > 0:
        array = steps_of(key, shape, pieces, -0.22, 0.18) * array
    return jnp.clip(array, min=-limit, max=limit).astype(kind)


def setup_inputs(seed: int = 0) -> dict:
    key_list = jax.random.split(jax.random.key(seed), 6)
    velocity = normal_values(key_list[0], (FIELDS, GRID_X, GRID_Y, GRID_Z), 1.0, 6.0, ((2, 8), (3, 4)), jnp.float32)
    coupling = normal_values(key_list[1], (FIELDS, FIELDS), 0.7, 4.0, (), jnp.float32)
    symbol_x = jnp.clip(jax.random.uniform(key_list[2], (GRID_X,), jnp.float32, 0.3, 3.0), 0.3, 3.0)
    symbol_y = jnp.clip(jax.random.uniform(key_list[3], (GRID_Y,), jnp.float32, 0.3, 3.0), 0.3, 3.0)
    symbol_z = jnp.clip(jax.random.uniform(key_list[4], (GRID_Z,), jnp.float32, 0.3, 3.0), 0.3, 3.0)
    return dict(velocity=velocity, coupling=coupling, symbol_x=symbol_x, symbol_y=symbol_y, symbol_z=symbol_z)


def basis_table(count):
    rank = jnp.arange(count)
    angle = (jnp.pi / (count + 1)) * (((rank[:, None] + 1) * (rank[None, :] + 1)) % (2 * count + 2)).astype(jnp.float32)
    return jnp.sin(angle) * (2.0 / (count + 1)) ** 0.5


def along_dim(values, dim):
    moved = jnp.tensordot(values, basis_table(values.shape[dim]), axes=([dim], [0]), precision=lax.Precision.HIGHEST)
    return jnp.moveaxis(moved, -1, dim)


def reference(velocity, coupling, symbol_x, symbol_y, symbol_z):
    spectrum = velocity
    spectrum = along_dim(spectrum, 1)
    spectrum = along_dim(spectrum, 2)
    spectrum = along_dim(spectrum, 3)
    symbol = symbol_x[:, None, None] + symbol_y[None, :, None] + symbol_z[None, None, :]
    weight_xyz = 1.0 / (1.0 + symbol)
    mixed_fields = jnp.einsum("ab,bxyz->axyz", coupling, spectrum, precision=lax.Precision.HIGHEST)
    spectrum = weight_xyz * spectrum + (1.0 - weight_xyz) * mixed_fields
    return spectrum
```

```python
import functools

import jax
import jax.numpy as jnp
import numpy as np
from jax import lax
from jax.experimental import pallas as pl
from jax.experimental.pallas import tpu as pltpu
from jax.sharding import PartitionSpec as P

LANES = 128
CHUNKS = 8
F32 = jnp.float32
BF16 = jnp.bfloat16
MESH = pl.DeviceIdType.MESH


def basis_table(count):
    rank = np.arange(1, count + 1)
    turns = (rank[:, None] * rank[None, :]) % (2 * count + 2)
    table = np.sin(np.pi / (count + 1) * turns) * (2.0 / (count + 1)) ** 0.5
    table = table.astype(np.float32)
    high = table.astype(jnp.bfloat16)
    low = (table - high.astype(np.float32)).astype(jnp.bfloat16)
    return high, low


def split(values):
    high = values.astype(BF16)
    low = (values - high.astype(F32)).astype(BF16)
    return high, low


def kernel(
    north, deep, chunks,
    a_hbm, coupling, sym_x, sym_y, sym_z, tx_hbm, ty_hbm, tz_hbm,
    out,
    a, tx, ty, tz, x1, r, s, t,
    load_sem, send_n, recv_n, send_d, recv_d,
):
    me_n = lax.axis_index("north")
    me_d = lax.axis_index("deep")
    fields, share_y, share_z, size_x = a.shape
    pack = LANES // share_z
    packs = fields // pack
    share_x = size_x // north
    size_y = share_y * north
    block_y = size_y // deep
    size_z = share_z * deep
    step = share_x // chunks
    half = deep // 2

    loads = [pltpu.make_async_copy(tx_hbm, tx, load_sem.at[0])]
    for p in range(packs):
        part = pl.ds(p * pack, pack)
        loads.append(pltpu.make_async_copy(a_hbm.at[part], a.at[part], load_sem.at[1 + p]))
    late = [
        pltpu.make_async_copy(ty_hbm, ty, load_sem.at[1 + packs]),
        pltpu.make_async_copy(tz_hbm, tz, load_sem.at[2 + packs]),
    ]
    for copy in loads + late:
        copy.start()

    peers_n = [lax.rem(me_n + k, north) for k in range(1, north)]
    side = me_d // half
    peers_d = [(1 - side) * half + lax.rem(me_d + j, half) for j in range(half)]
    peers_d += [side * half + lax.rem(me_d + j, half) for j in range(1, half)]

    barrier = pltpu.get_barrier_semaphore()
    for peer in peers_n:
        pl.semaphore_signal(barrier, inc=1, device_id={"north": peer}, device_id_type=MESH)
    for peer in peers_d:
        pl.semaphore_signal(barrier, inc=1, device_id={"deep": peer}, device_id_type=MESH)

    loads[0].wait()
    for p in range(packs):
        loads[1 + p].wait()
        for y in range(share_y):
            rows = jnp.concatenate([a[p * pack + f, y] for f in range(pack)], axis=0)
            high, low = split(rows)
            dot = functools.partial(
                lax.dot_general,
                dimension_numbers=(((1,), (1,)), ((), ())),
                preferred_element_type=F32,
            )
            x1[p, :, y, :] = dot(tx[0], high) + dot(tx[1], high) + dot(tx[0], low)

    pl.semaphore_wait(barrier, len(peers_n) + len(peers_d))

    def north_copy(c, peer, slot):
        return pltpu.make_async_remote_copy(
            src_ref=x1.at[:, pl.ds(peer * share_x + c * step, step)],
            dst_ref=r.at[:, pl.ds(c * step, step), pl.ds(pl.multiple_of(me_n * share_y, 8), share_y)],
            send_sem=send_n.at[c, slot],
            recv_sem=recv_n.at[c, slot],
            device_id={"north": peer},
            device_id_type=MESH,
        )

    def deep_copy(c, peer, source):
        return pltpu.make_async_remote_copy(
            src_ref=s.at[:, pl.ds(c * step, step), pl.ds(pl.multiple_of(peer * block_y, 8), block_y)],
            dst_ref=t.at[me_d, :, pl.ds(c * step, step)],
            send_sem=send_d.at[c, peer],
            recv_sem=recv_d.at[c, source],
            device_id={"deep": peer},
            device_id_type=MESH,
        )

    for c in range(chunks):
        for slot, peer in enumerate(peers_n):
            north_copy(c, peer, slot).start()

    own_rows = pl.ds(pl.multiple_of(me_n * share_y, 8), share_y)
    r[:, :, own_rows, :] = x1[:, pl.ds(me_n * share_x, share_x)]

    rows_y = lax.broadcasted_iota(jnp.int32, (block_y, size_z), 0)
    base = jnp.broadcast_to(sym_z[...], (block_y, size_z))
    column = jnp.zeros((block_y, size_z), F32)
    for i in range(block_y):
        column = jnp.where(rows_y == i, sym_y[me_d * block_y + i], column)
    base = base + column

    for copy in late:
        copy.wait()

    for c in range(chunks):
        for slot, peer in enumerate(peers_n):
            north_copy(c, peer, slot).wait_recv()
        for p in range(packs):
            for x in range(c * step, (c + 1) * step, 2):
                width = min(2, (c + 1) * step - x)
                high, low = split(jnp.concatenate([r[p, x + i] for i in range(width)], axis=1))
                stack = jnp.concatenate([high, high, low], axis=0)
                mixed = jnp.dot(ty[...], stack, preferred_element_type=F32)
                for i in range(width):
                    s[p, x + i] = mixed[:, i * LANES:(i + 1) * LANES]
        for peer in peers_d:
            deep_copy(c, peer, me_d).start()

    own_block = pl.ds(pl.multiple_of(me_d * block_y, 8), block_y)
    t[me_d] = s[:, :, own_block, :]

    for c in range(chunks):
        for peer in peers_d:
            deep_copy(c, peer, peer).wait_recv()
        spectrum = []
        for p in range(packs):
            parts = [
                t[d, p, c * step:(c + 1) * step].reshape(step * block_y, LANES)
                for d in range(deep)
            ]
            for f in range(pack):
                rows = jnp.concatenate(
                    [part[:, f * share_z:(f + 1) * share_z] for part in parts], axis=1
                )
                high, low = split(rows)
                spectrum.append(
                    jnp.dot(high, tz[0], preferred_element_type=F32)
                    + jnp.dot(high, tz[1], preferred_element_type=F32)
                    + jnp.dot(low, tz[0], preferred_element_type=F32)
                )
        for i in range(step):
            x = c * step + i
            weight = 1.0 / (1.0 + (base + sym_x[me_n * share_x + x]))
            rest = 1.0 - weight
            old = [value[i * block_y:(i + 1) * block_y] for value in spectrum]
            for f in range(fields):
                total = coupling[f, 0] * old[0]
                for g in range(1, fields):
                    total = total + coupling[f, g] * old[g]
                out[f, x] = weight * old[f] + rest * total

    for c in range(chunks):
        for slot, peer in enumerate(peers_n):
            north_copy(c, peer, slot).wait_send()
        for peer in peers_d:
            deep_copy(c, peer, me_d).wait_send()


def on_device(north, deep, velocity, coupling, symbol_x, symbol_y, symbol_z):
    field = jnp.transpose(velocity, (0, 2, 3, 1))
    fields, share_y, share_z, size_x = field.shape
    size_y, size_z = share_y * north, share_z * deep
    share_x, block_y = size_x // north, size_y // deep
    packs = fields * share_z // LANES
    chunks = min(CHUNKS, share_x)
    high, low = basis_table(size_x)
    tx = jnp.asarray(np.stack([high, low]))
    high, low = basis_table(size_y)
    ty = jnp.asarray(np.concatenate([high, low, high], axis=1))
    high, low = basis_table(size_z)
    tz = jnp.asarray(np.stack([high, low]))
    smem = pl.BlockSpec(memory_space=pltpu.SMEM)
    vmem = pl.BlockSpec(memory_space=pltpu.VMEM)
    hbm = pl.BlockSpec(memory_space=pl.ANY)
    return pl.pallas_call(
        functools.partial(kernel, north, deep, chunks),
        out_shape=jax.ShapeDtypeStruct((fields, share_x, block_y, size_z), F32),
        in_specs=[hbm, smem, smem, smem, vmem, hbm, hbm, hbm],
        out_specs=vmem,
        scratch_shapes=[
            pltpu.VMEM(field.shape, F32),
            pltpu.VMEM(tx.shape, BF16),
            pltpu.VMEM(ty.shape, BF16),
            pltpu.VMEM(tz.shape, BF16),
            pltpu.VMEM((packs, size_x, share_y, LANES), F32),
            pltpu.VMEM((packs, share_x, size_y, LANES), F32),
            pltpu.VMEM((packs, share_x, size_y, LANES), F32),
            pltpu.VMEM((deep, packs, share_x, block_y, LANES), F32),
            pltpu.SemaphoreType.DMA((3 + packs,)),
            pltpu.SemaphoreType.DMA((chunks, north - 1)),
            pltpu.SemaphoreType.DMA((chunks, north - 1)),
            pltpu.SemaphoreType.DMA((chunks, deep)),
            pltpu.SemaphoreType.DMA((chunks, deep)),
        ],
        compiler_params=pltpu.CompilerParams(collective_id=0, has_side_effects=True),
    )(field, coupling, symbol_x, symbol_y, symbol_z[None, :], tx, ty, tz)


def solution(mesh):
    placed = (P(None, None, "north", "deep"), P(), P(), P(), P())
    return jax.shard_map(
        functools.partial(on_device, mesh.shape["north"], mesh.shape["deep"]),
        mesh=mesh,
        in_specs=placed,
        out_specs=P(None, "north", "deep", None),
        check_vma=False,
    )
```

```python
import functools

import jax
import jax.numpy as jnp
import numpy as np
from jax import lax
from jax.experimental import pallas as pl
from jax.experimental.pallas import tpu as pltpu
from jax.sharding import PartitionSpec as P

LANES = 128
CHUNKS = 8
F32 = jnp.float32
BF16 = jnp.bfloat16
MESH = pl.DeviceIdType.MESH


def basis_table(count):
    rank = np.arange(1, count + 1)
    turns = (rank[:, None] * rank[None, :]) % (2 * count + 2)
    table = np.sin(np.pi / (count + 1) * turns) * (2.0 / (count + 1)) ** 0.5
    table = table.astype(np.float32)
    high = table.astype(jnp.bfloat16)
    low = (table - high.astype(np.float32)).astype(jnp.bfloat16)
    return high, low


def split(values):
    high = values.astype(BF16)
    low = (values - high.astype(F32)).astype(BF16)
    return high, low


def kernel(
    north, deep, chunks,
    a_hbm, coupling_hbm, sym_x_hbm, sym_y_hbm, sym_z_hbm, tx_hbm, ty_hbm, tz_hbm,
    out,
    a, coupling, sym_x, sym_y, sym_z, tx, ty, tz, x1, r, s, t,
    load_sem, send_n, recv_n, send_d, recv_d,
):
    me_n = lax.axis_index("north")
    me_d = lax.axis_index("deep")
    fields, share_y, share_z, size_x = a.shape
    pack = LANES // share_z
    packs = fields // pack
    share_x = size_x // north
    size_y = share_y * north
    block_y = size_y // deep
    size_z = share_z * deep
    step = share_x // chunks
    half = deep // 2

    loads = [pltpu.make_async_copy(tx_hbm, tx, load_sem.at[0])]
    for p in range(packs):
        part = pl.ds(p * pack, pack)
        loads.append(pltpu.make_async_copy(a_hbm.at[part], a.at[part], load_sem.at[1 + p]))
    pairs = [
        (ty_hbm, ty), (sym_x_hbm, sym_x), (sym_y_hbm, sym_y), (sym_z_hbm, sym_z),
        (coupling_hbm, coupling), (tz_hbm, tz),
    ]
    late = [
        pltpu.make_async_copy(source, target, load_sem.at[1 + packs + i])
        for i, (source, target) in enumerate(pairs)
    ]
    for copy in loads + late:
        copy.start()

    peers_n = [lax.rem(me_n + k, north) for k in range(1, north)]
    side = me_d // half
    peers_d = [(1 - side) * half + lax.rem(me_d + j, half) for j in range(half)]
    peers_d += [side * half + lax.rem(me_d + j, half) for j in range(1, half)]

    barrier = pltpu.get_barrier_semaphore()
    for peer in peers_n:
        pl.semaphore_signal(barrier, inc=1, device_id={"north": peer}, device_id_type=MESH)
    for peer in peers_d:
        pl.semaphore_signal(barrier, inc=1, device_id={"deep": peer}, device_id_type=MESH)

    loads[0].wait()
    for p in range(packs):
        loads[1 + p].wait()
        for y in range(0, share_y, 2):
            rows = [a[p * pack + f, y + i] for i in range(2) for f in range(pack)]
            high, low = split(jnp.concatenate(rows, axis=0))
            lines = lax.dot_general(
                tx[...],
                jnp.concatenate([high, high, low], axis=1),
                dimension_numbers=(((1,), (1,)), ((), ())),
                preferred_element_type=F32,
            )
            x1[p, :, y, :] = lines[:, :LANES]
            x1[p, :, y + 1, :] = lines[:, LANES:]

    pl.semaphore_wait(barrier, len(peers_n) + len(peers_d))

    def north_copy(c, peer, slot):
        return pltpu.make_async_remote_copy(
            src_ref=x1.at[:, pl.ds(peer * share_x + c * step, step)],
            dst_ref=r.at[:, pl.ds(c * step, step), pl.ds(pl.multiple_of(me_n * share_y, 8), share_y)],
            send_sem=send_n.at[c, slot],
            recv_sem=recv_n.at[c, slot],
            device_id={"north": peer},
            device_id_type=MESH,
        )

    def deep_copy(c, peer, source):
        return pltpu.make_async_remote_copy(
            src_ref=s.at[:, pl.ds(c * step, step), pl.ds(pl.multiple_of(peer * block_y, 8), block_y)],
            dst_ref=t.at[me_d, :, pl.ds(c * step, step)],
            send_sem=send_d.at[c, peer],
            recv_sem=recv_d.at[c, source],
            device_id={"deep": peer},
            device_id_type=MESH,
        )

    for c in range(chunks):
        for slot, peer in enumerate(peers_n):
            north_copy(c, peer, slot).start()

    own_rows = pl.ds(pl.multiple_of(me_n * share_y, 8), share_y)
    r[:, :, own_rows, :] = x1[:, pl.ds(me_n * share_x, share_x)]

    for copy in late:
        copy.wait()

    rows_y = lax.broadcasted_iota(jnp.int32, (block_y, size_z), 0)
    base = jnp.broadcast_to(sym_z[...], (block_y, size_z))
    column = jnp.zeros((block_y, size_z), F32)
    for i in range(block_y):
        column = jnp.where(rows_y == i, sym_y[0, me_d * block_y + i], column)
    base = base + column

    for c in range(chunks):
        for slot, peer in enumerate(peers_n):
            north_copy(c, peer, slot).wait_recv()
        for p in range(packs):
            for x in range(c * step, (c + 1) * step, 2):
                width = min(2, (c + 1) * step - x)
                high, low = split(jnp.concatenate([r[p, x + i] for i in range(width)], axis=1))
                stack = jnp.concatenate([high, high, low], axis=0)
                mixed = jnp.dot(ty[...], stack, preferred_element_type=F32)
                for i in range(width):
                    s[p, x + i] = mixed[:, i * LANES:(i + 1) * LANES]
        for peer in peers_d:
            deep_copy(c, peer, me_d).start()

    own_block = pl.ds(pl.multiple_of(me_d * block_y, 8), block_y)
    t[me_d] = s[:, :, own_block, :]

    for c in range(chunks):
        for peer in peers_d:
            deep_copy(c, peer, peer).wait_recv()
        spectrum = []
        for p in range(packs):
            parts = [
                t[d, p, c * step:(c + 1) * step].reshape(step * block_y, LANES)
                for d in range(deep)
            ]
            for f in range(pack):
                rows = jnp.concatenate(
                    [part[:, f * share_z:(f + 1) * share_z] for part in parts], axis=1
                )
                high, low = split(rows)
                spectrum.append(
                    jnp.dot(high, tz[0], preferred_element_type=F32)
                    + jnp.dot(high, tz[1], preferred_element_type=F32)
                    + jnp.dot(low, tz[0], preferred_element_type=F32)
                )
        for i in range(step):
            x = c * step + i
            weight = 1.0 / (1.0 + (base + sym_x[0, me_n * share_x + x]))
            rest = 1.0 - weight
            old = [value[i * block_y:(i + 1) * block_y] for value in spectrum]
            for f in range(fields):
                total = coupling[f, 0] * old[0]
                for g in range(1, fields):
                    total = total + coupling[f, g] * old[g]
                out[f, x] = weight * old[f] + rest * total

    for c in range(chunks):
        for slot, peer in enumerate(peers_n):
            north_copy(c, peer, slot).wait_send()
        for peer in peers_d:
            deep_copy(c, peer, me_d).wait_send()


def on_device(north, deep, velocity, coupling, symbol_x, symbol_y, symbol_z):
    field = jnp.transpose(velocity, (0, 2, 3, 1))
    fields, share_y, share_z, size_x = field.shape
    size_y, size_z = share_y * north, share_z * deep
    share_x, block_y = size_x // north, size_y // deep
    packs = fields * share_z // LANES
    chunks = min(CHUNKS, share_x)
    high, low = basis_table(size_x)
    tx = jnp.asarray(np.concatenate([high, low, high], axis=1))
    high, low = basis_table(size_y)
    ty = jnp.asarray(np.concatenate([high, low, high], axis=1))
    high, low = basis_table(size_z)
    tz = jnp.asarray(np.stack([high, low]))
    need = 4 * field.size * 7 + 2 * (tx.size + ty.size + tz.size) + 2**21
    vmem = pl.BlockSpec(memory_space=pltpu.VMEM)
    hbm = pl.BlockSpec(memory_space=pltpu.HBM)
    operands = (field, coupling, symbol_x[None, :], symbol_y[None, :], symbol_z[None, :], tx, ty, tz)
    return pl.pallas_call(
        functools.partial(kernel, north, deep, chunks),
        out_shape=jax.ShapeDtypeStruct((fields, share_x, block_y, size_z), F32),
        in_specs=[hbm] * 8,
        out_specs=vmem,
        scratch_shapes=[
            pltpu.VMEM(field.shape, F32),
            pltpu.SMEM(coupling.shape, F32),
            pltpu.SMEM((1, size_x), F32),
            pltpu.SMEM((1, size_y), F32),
            pltpu.VMEM((1, size_z), F32),
            pltpu.VMEM(tx.shape, BF16),
            pltpu.VMEM(ty.shape, BF16),
            pltpu.VMEM(tz.shape, BF16),
            pltpu.VMEM((packs, size_x, share_y, LANES), F32),
            pltpu.VMEM((packs, share_x, size_y, LANES), F32),
            pltpu.VMEM((packs, share_x, size_y, LANES), F32),
            pltpu.VMEM((deep, packs, share_x, block_y, LANES), F32),
            pltpu.SemaphoreType.DMA((7 + packs,)),
            pltpu.SemaphoreType.DMA((chunks, north - 1)),
            pltpu.SemaphoreType.DMA((chunks, north - 1)),
            pltpu.SemaphoreType.DMA((chunks, deep)),
            pltpu.SemaphoreType.DMA((chunks, deep)),
        ],
        compiler_params=pltpu.CompilerParams(
            collective_id=0, has_side_effects=True, vmem_limit_bytes=need
        ),
    )(*[pltpu.with_memory_space_constraint(v, pltpu.HBM) for v in operands])


def solution(mesh):
    placed = (P(None, None, "north", "deep"), P(), P(), P(), P())
    return jax.shard_map(
        functools.partial(on_device, mesh.shape["north"], mesh.shape["deep"]),
        mesh=mesh,
        in_specs=placed,
        out_specs=P(None, "north", "deep", None),
        check_vma=False,
    )
```

```python
import functools

import jax
import jax.numpy as jnp
import numpy as np
from jax import lax
from jax.experimental import pallas as pl
from jax.experimental.pallas import tpu as pltpu
from jax.sharding import PartitionSpec as P

LANES = 128
SIZES = (3, 5, 8)
F32 = jnp.float32
BF16 = jnp.bfloat16
MESH = pl.DeviceIdType.MESH


def basis_table(count):
    rank = np.arange(1, count + 1)
    turns = (rank[:, None] * rank[None, :]) % (2 * count + 2)
    table = np.sin(np.pi / (count + 1) * turns) * (2.0 / (count + 1)) ** 0.5
    table = table.astype(np.float32)
    high = table.astype(jnp.bfloat16)
    low = (table - high.astype(np.float32)).astype(jnp.bfloat16)
    return high, low


def split(values):
    high = values.astype(BF16)
    low = (values - high.astype(F32)).astype(BF16)
    return high, low


def kernel(
    north, deep, chunks,
    a_hbm, coupling_hbm, sym_x_hbm, sym_y_hbm, sym_z_hbm, tx_hbm, ty_hbm, tz_hbm,
    out,
    a, coupling, sym_x, sym_y, sym_z, tx, ty, tz, x1, r, s, t,
    load_sem, send_n, recv_n, send_d, recv_d,
):
    me_n = lax.axis_index("north")
    me_d = lax.axis_index("deep")
    fields, share_y, share_z, size_x = a.shape
    pack = LANES // share_z
    packs = fields // pack
    share_x = size_x // north
    size_y = share_y * north
    block_y = size_y // deep
    size_z = share_z * deep
    starts = [sum(chunks[:c]) for c in range(len(chunks))]
    pieces = [(p, 1, starts[0], chunks[0]) for p in range(packs)]
    pieces += [(0, packs, starts[c], chunks[c]) for c in range(1, len(chunks))]
    half = deep // 2

    loads = [pltpu.make_async_copy(tx_hbm, tx, load_sem.at[0])]
    for p in range(packs):
        part = pl.ds(p * pack, pack)
        loads.append(pltpu.make_async_copy(a_hbm.at[part], a.at[part], load_sem.at[1 + p]))
    pairs = [
        (ty_hbm, ty), (sym_x_hbm, sym_x), (sym_y_hbm, sym_y), (sym_z_hbm, sym_z),
        (coupling_hbm, coupling), (tz_hbm, tz),
    ]
    late = [
        pltpu.make_async_copy(source, target, load_sem.at[1 + packs + i])
        for i, (source, target) in enumerate(pairs)
    ]
    for copy in loads + late:
        copy.start()

    peers_n = [lax.rem(me_n + k, north) for k in range(1, north)]
    side = me_d // half
    peers_d = [(1 - side) * half + lax.rem(me_d + j, half) for j in range(half)]
    peers_d += [side * half + lax.rem(me_d + j, half) for j in range(1, half)]

    barrier = pltpu.get_barrier_semaphore()
    for peer in peers_n:
        pl.semaphore_signal(barrier, inc=1, device_id={"north": peer}, device_id_type=MESH)
    for peer in peers_d:
        pl.semaphore_signal(barrier, inc=1, device_id={"deep": peer}, device_id_type=MESH)

    def north_copy(c, peer, slot):
        p, count, x, size = pieces[c]
        return pltpu.make_async_remote_copy(
            src_ref=x1.at[pl.ds(peer * share_x + x, size), pl.ds(p, count)],
            dst_ref=r.at[me_n, pl.ds(x, size), pl.ds(p, count)],
            send_sem=send_n.at[c, slot],
            recv_sem=recv_n.at[c, slot],
            device_id={"north": peer},
            device_id_type=MESH,
        )

    def deep_copy(c, peer, source):
        p, count, x, size = pieces[c]
        return pltpu.make_async_remote_copy(
            src_ref=s.at[peer, pl.ds(x, size), pl.ds(p, count)],
            dst_ref=t.at[me_d, pl.ds(x, size), pl.ds(p, count)],
            send_sem=send_d.at[c, peer],
            recv_sem=recv_d.at[c, source],
            device_id={"deep": peer},
            device_id_type=MESH,
        )

    loads[0].wait()
    for p in range(packs):
        loads[1 + p].wait()
        for y in range(0, share_y, 2):
            rows = [a[p * pack + f, y + i] for i in range(2) for f in range(pack)]
            high, low = split(jnp.concatenate(rows, axis=0))
            lines = lax.dot_general(
                tx[...],
                jnp.concatenate([high, high, low], axis=1),
                dimension_numbers=(((1,), (1,)), ((), ())),
                preferred_element_type=F32,
            )
            x1[:, p, y, :] = lines[:, :LANES]
            x1[:, p, y + 1, :] = lines[:, LANES:]
        if p == 0:
            pl.semaphore_wait(barrier, len(peers_n) + len(peers_d))
        for slot, peer in enumerate(peers_n):
            north_copy(p, peer, slot).start()

    for c in range(packs, len(pieces)):
        for slot, peer in enumerate(peers_n):
            north_copy(c, peer, slot).start()

    r[me_n] = x1[pl.ds(me_n * share_x, share_x)]

    for copy in late:
        copy.wait()

    rows_y = lax.broadcasted_iota(jnp.int32, (block_y, size_z), 0)
    base = jnp.broadcast_to(sym_z[...], (block_y, size_z))
    column = jnp.zeros((block_y, size_z), F32)
    for i in range(block_y):
        column = jnp.where(rows_y == i, sym_y[0, me_d * block_y + i], column)
    base = base + column

    for c in range(len(pieces)):
        first, count, start, size = pieces[c]
        for slot, peer in enumerate(peers_n):
            north_copy(c, peer, slot).wait_recv()
        for p in range(first, first + count):
            for x in range(start, start + size, 2):
                width = min(2, start + size - x)
                lines = [
                    jnp.concatenate([r[n, x + i, p] for n in range(north)], axis=0)
                    for i in range(width)
                ]
                high, low = split(jnp.concatenate(lines, axis=1))
                stack = jnp.concatenate([high, high, low], axis=0)
                mixed = jnp.dot(ty[...], stack, preferred_element_type=F32)
                for i in range(width):
                    modes = mixed[:, i * LANES:(i + 1) * LANES]
                    for d in range(deep):
                        s[d, x + i, p] = modes[d * block_y:(d + 1) * block_y]
        for peer in peers_d:
            deep_copy(c, peer, me_d).start()

    t[me_d] = s[me_d]

    for c in range(len(chunks)):
        for k in range(packs) if c == 0 else [packs + c - 1]:
            for peer in peers_d:
                deep_copy(k, peer, peer).wait_recv()
        spectrum = []
        for p in range(packs):
            parts = [
                t[d, starts[c]:starts[c] + chunks[c], p].reshape(chunks[c] * block_y, LANES)
                for d in range(deep)
            ]
            for f in range(pack):
                rows = jnp.concatenate(
                    [part[:, f * share_z:(f + 1) * share_z] for part in parts], axis=1
                )
                high, low = split(rows)
                spectrum.append(
                    jnp.dot(high, tz[0], preferred_element_type=F32)
                    + jnp.dot(high, tz[1], preferred_element_type=F32)
                    + jnp.dot(low, tz[0], preferred_element_type=F32)
                )
        for i in range(chunks[c]):
            x = starts[c] + i
            weight = 1.0 / (1.0 + (base + sym_x[0, me_n * share_x + x]))
            rest = 1.0 - weight
            old = [value[i * block_y:(i + 1) * block_y] for value in spectrum]
            for f in range(fields):
                total = coupling[f, 0] * old[0]
                for g in range(1, fields):
                    total = total + coupling[f, g] * old[g]
                out[f, x] = weight * old[f] + rest * total

    for c in range(len(pieces)):
        for slot, peer in enumerate(peers_n):
            north_copy(c, peer, slot).wait_send()
        for peer in peers_d:
            deep_copy(c, peer, me_d).wait_send()


def on_device(north, deep, velocity, coupling, symbol_x, symbol_y, symbol_z):
    field = jnp.transpose(velocity, (0, 2, 3, 1))
    fields, share_y, share_z, size_x = field.shape
    size_y, size_z = share_y * north, share_z * deep
    share_x, block_y = size_x // north, size_y // deep
    packs = fields * share_z // LANES
    unit = sum(SIZES)
    chunks = [size * share_x // unit for size in SIZES] if share_x % unit == 0 else [share_x]
    high, low = basis_table(size_x)
    tx = jnp.asarray(np.concatenate([high, low, high], axis=1))
    high, low = basis_table(size_y)
    ty = jnp.asarray(np.concatenate([high, low, high], axis=1))
    high, low = basis_table(size_z)
    tz = jnp.asarray(np.stack([high, low]))
    need = 4 * field.size * 7 + 2 * (tx.size + ty.size + tz.size) + 2**21
    vmem = pl.BlockSpec(memory_space=pltpu.VMEM)
    hbm = pl.BlockSpec(memory_space=pltpu.HBM)
    operands = (field, coupling, symbol_x[None, :], symbol_y[None, :], symbol_z[None, :], tx, ty, tz)
    return pl.pallas_call(
        functools.partial(kernel, north, deep, chunks),
        out_shape=jax.ShapeDtypeStruct((fields, share_x, block_y, size_z), F32),
        in_specs=[hbm] * 8,
        out_specs=vmem,
        scratch_shapes=[
            pltpu.VMEM(field.shape, F32),
            pltpu.SMEM(coupling.shape, F32),
            pltpu.SMEM((1, size_x), F32),
            pltpu.SMEM((1, size_y), F32),
            pltpu.VMEM((1, size_z), F32),
            pltpu.VMEM(tx.shape, BF16),
            pltpu.VMEM(ty.shape, BF16),
            pltpu.VMEM(tz.shape, BF16),
            pltpu.VMEM((size_x, packs, share_y, LANES), F32),
            pltpu.VMEM((north, share_x, packs, share_y, LANES), F32),
            pltpu.VMEM((deep, share_x, packs, block_y, LANES), F32),
            pltpu.VMEM((deep, share_x, packs, block_y, LANES), F32),
            pltpu.SemaphoreType.DMA((7 + packs,)),
            pltpu.SemaphoreType.DMA((len(chunks) + packs - 1, north - 1)),
            pltpu.SemaphoreType.DMA((len(chunks) + packs - 1, north - 1)),
            pltpu.SemaphoreType.DMA((len(chunks) + packs - 1, deep)),
            pltpu.SemaphoreType.DMA((len(chunks) + packs - 1, deep)),
        ],
        compiler_params=pltpu.CompilerParams(
            collective_id=0, has_side_effects=True, vmem_limit_bytes=need
        ),
    )(*[pltpu.with_memory_space_constraint(v, pltpu.HBM) for v in operands])


def solution(mesh):
    placed = (P(None, None, "north", "deep"), P(), P(), P(), P())
    return jax.shard_map(
        functools.partial(on_device, mesh.shape["north"], mesh.shape["deep"]),
        mesh=mesh,
        in_specs=placed,
        out_specs=P(None, "north", "deep", None),
        check_vma=False,
    )
```

```python
import functools

import jax
import jax.numpy as jnp
import numpy as np
from jax import lax
from jax.experimental import pallas as pl
from jax.experimental.pallas import tpu as pltpu
from jax.sharding import PartitionSpec as P

LANES = 128
SIZES = (3, 5, 8)
F32 = jnp.float32
BF16 = jnp.bfloat16
MESH = pl.DeviceIdType.MESH


def basis_table(count):
    rank = np.arange(1, count + 1)
    turns = (rank[:, None] * rank[None, :]) % (2 * count + 2)
    table = np.sin(np.pi / (count + 1) * turns) * (2.0 / (count + 1)) ** 0.5
    table = table.astype(np.float32)
    high = table.astype(jnp.bfloat16)
    low = (table - high.astype(np.float32)).astype(jnp.bfloat16)
    return high, low


def split(values):
    high = values.astype(BF16)
    low = (values - high.astype(F32)).astype(BF16)
    return high, low


def kernel(
    north, deep, chunks,
    a_hbm, coupling_hbm, sym_x_hbm, sym_y_hbm, sym_z_hbm, tx_hbm, ty_hbm, tz_hbm,
    out,
    a, coupling, sym_x, sym_y, sym_z, tx, ty, tz, x1, r, s, t,
    load_sem, send_n, recv_n, send_d, recv_d,
):
    me_n = lax.axis_index("north")
    me_d = lax.axis_index("deep")
    fields, share_y, share_z, size_x = a.shape
    pack = LANES // share_z
    packs = fields // pack
    share_x = size_x // north
    size_y = share_y * north
    block_y = size_y // deep
    size_z = share_z * deep
    starts = [sum(chunks[:c]) for c in range(len(chunks))]
    pieces = []
    for c in range(len(chunks)):
        count = 1 if c in (0, len(chunks) - 1) else packs
        pieces += [(p, count, starts[c], chunks[c]) for p in range(0, packs, count)]
    half = deep // 2

    peers_n = [lax.rem(me_n + k, north) for k in range(1, north)]
    side = me_d // half
    peers_d = [(1 - side) * half + lax.rem(me_d + j, half) for j in range(half)]
    peers_d += [side * half + lax.rem(me_d + j, half) for j in range(1, half)]

    barrier = pltpu.get_barrier_semaphore()
    for peer in peers_n:
        pl.semaphore_signal(barrier, inc=1, device_id={"north": peer}, device_id_type=MESH)
    for peer in peers_d:
        pl.semaphore_signal(barrier, inc=1, device_id={"deep": peer}, device_id_type=MESH)

    loads = [pltpu.make_async_copy(tx_hbm, tx, load_sem.at[0])]
    for p in range(packs):
        part = pl.ds(p * pack, pack)
        loads.append(pltpu.make_async_copy(a_hbm.at[part], a.at[part], load_sem.at[1 + p]))
    pairs = [
        (ty_hbm, ty), (sym_x_hbm, sym_x), (sym_y_hbm, sym_y), (sym_z_hbm, sym_z),
        (coupling_hbm, coupling), (tz_hbm, tz),
    ]
    late = [
        pltpu.make_async_copy(source, target, load_sem.at[1 + packs + i])
        for i, (source, target) in enumerate(pairs)
    ]
    for copy in loads:
        copy.start()

    def north_copy(c, peer, slot):
        p, count, x, size = pieces[c]
        return pltpu.make_async_remote_copy(
            src_ref=x1.at[pl.ds(peer * share_x + x, size), pl.ds(p, count)],
            dst_ref=r.at[me_n, pl.ds(x, size), pl.ds(p, count)],
            send_sem=send_n.at[c, slot],
            recv_sem=recv_n.at[c, slot],
            device_id={"north": peer},
            device_id_type=MESH,
        )

    def deep_copy(c, peer, source):
        p, count, x, size = pieces[c]
        return pltpu.make_async_remote_copy(
            src_ref=s.at[peer, pl.ds(x, size), pl.ds(p, count)],
            dst_ref=t.at[me_d, pl.ds(x, size), pl.ds(p, count)],
            send_sem=send_d.at[c, peer],
            recv_sem=recv_d.at[c, source],
            device_id={"deep": peer},
            device_id_type=MESH,
        )

    loads[0].wait()
    for p in range(packs):
        loads[1 + p].wait()
        for y in range(0, share_y, 2):
            rows = [a[p * pack + f, y + i] for i in range(2) for f in range(pack)]
            high, low = split(jnp.concatenate(rows, axis=0))
            lines = lax.dot_general(
                tx[...],
                jnp.concatenate([high, high, low], axis=1),
                dimension_numbers=(((1,), (1,)), ((), ())),
                preferred_element_type=F32,
            )
            x1[:, p, y, :] = lines[:, :LANES]
            x1[:, p, y + 1, :] = lines[:, LANES:]
        if p == 0:
            pl.semaphore_wait(barrier, len(peers_n) + len(peers_d))
        for slot, peer in enumerate(peers_n):
            north_copy(p, peer, slot).start()
    for copy in late:
        copy.start()

    for c in range(packs, len(pieces)):
        for slot, peer in enumerate(peers_n):
            north_copy(c, peer, slot).start()

    r[me_n] = x1[pl.ds(me_n * share_x, share_x)]

    for copy in late:
        copy.wait()

    rows_y = lax.broadcasted_iota(jnp.int32, (block_y, size_z), 0)
    base = jnp.broadcast_to(sym_z[...], (block_y, size_z))
    column = jnp.zeros((block_y, size_z), F32)
    for i in range(block_y):
        column = jnp.where(rows_y == i, sym_y[0, me_d * block_y + i], column)
    base = base + column

    for c in range(len(pieces)):
        first, count, start, size = pieces[c]
        for slot, peer in enumerate(peers_n):
            north_copy(c, peer, slot).wait_recv()
        for p in range(first, first + count):
            for x in range(start, start + size, 2):
                width = min(2, start + size - x)
                lines = [
                    jnp.concatenate([r[n, x + i, p] for n in range(north)], axis=0)
                    for i in range(width)
                ]
                high, low = split(jnp.concatenate(lines, axis=1))
                stack = jnp.concatenate([high, high, low], axis=0)
                mixed = jnp.dot(ty[...], stack, preferred_element_type=F32)
                for i in range(width):
                    modes = mixed[:, i * LANES:(i + 1) * LANES]
                    for d in range(deep):
                        s[d, x + i, p] = modes[d * block_y:(d + 1) * block_y]
        for peer in peers_d:
            deep_copy(c, peer, me_d).start()

    t[me_d] = s[me_d]

    for c in range(len(chunks)):
        spectrum = []
        for p in range(packs):
            for k, (first, _, start, _) in enumerate(pieces):
                if start == starts[c] and first == p:
                    for peer in peers_d:
                        deep_copy(k, peer, peer).wait_recv()
            parts = [
                t[d, starts[c]:starts[c] + chunks[c], p].reshape(chunks[c] * block_y, LANES)
                for d in range(deep)
            ]
            for f in range(pack):
                rows = jnp.concatenate(
                    [part[:, f * share_z:(f + 1) * share_z] for part in parts], axis=1
                )
                high, low = split(rows)
                spectrum.append(
                    jnp.dot(high, tz[0], preferred_element_type=F32)
                    + jnp.dot(high, tz[1], preferred_element_type=F32)
                    + jnp.dot(low, tz[0], preferred_element_type=F32)
                )
        for i in range(chunks[c]):
            x = starts[c] + i
            weight = 1.0 / (1.0 + (base + sym_x[0, me_n * share_x + x]))
            rest = 1.0 - weight
            old = [value[i * block_y:(i + 1) * block_y] for value in spectrum]
            for f in range(fields):
                total = coupling[f, 0] * old[0]
                for g in range(1, fields):
                    total = total + coupling[f, g] * old[g]
                out[f, x] = weight * old[f] + rest * total

    for c in range(len(pieces)):
        for slot, peer in enumerate(peers_n):
            north_copy(c, peer, slot).wait_send()
        for peer in peers_d:
            deep_copy(c, peer, me_d).wait_send()


def on_device(north, deep, velocity, coupling, symbol_x, symbol_y, symbol_z):
    field = jnp.transpose(velocity, (0, 2, 3, 1))
    fields, share_y, share_z, size_x = field.shape
    size_y, size_z = share_y * north, share_z * deep
    share_x, block_y = size_x // north, size_y // deep
    packs = fields * share_z // LANES
    unit = sum(SIZES)
    chunks = [size * share_x // unit for size in SIZES] if share_x % unit == 0 else [share_x]
    high, low = basis_table(size_x)
    tx = jnp.asarray(np.concatenate([high, low, high], axis=1))
    high, low = basis_table(size_y)
    ty = jnp.asarray(np.concatenate([high, low, high], axis=1))
    high, low = basis_table(size_z)
    tz = jnp.asarray(np.stack([high, low]))
    need = 4 * field.size * 7 + 2 * (tx.size + ty.size + tz.size) + 2**21
    vmem = pl.BlockSpec(memory_space=pltpu.VMEM)
    hbm = pl.BlockSpec(memory_space=pltpu.HBM)
    operands = (field, coupling, symbol_x[None, :], symbol_y[None, :], symbol_z[None, :], tx, ty, tz)
    return pl.pallas_call(
        functools.partial(kernel, north, deep, chunks),
        out_shape=jax.ShapeDtypeStruct((fields, share_x, block_y, size_z), F32),
        in_specs=[hbm] * 8,
        out_specs=vmem,
        scratch_shapes=[
            pltpu.VMEM(field.shape, F32),
            pltpu.SMEM(coupling.shape, F32),
            pltpu.SMEM((1, size_x), F32),
            pltpu.SMEM((1, size_y), F32),
            pltpu.VMEM((1, size_z), F32),
            pltpu.VMEM(tx.shape, BF16),
            pltpu.VMEM(ty.shape, BF16),
            pltpu.VMEM(tz.shape, BF16),
            pltpu.VMEM((size_x, packs, share_y, LANES), F32),
            pltpu.VMEM((north, share_x, packs, share_y, LANES), F32),
            pltpu.VMEM((deep, share_x, packs, block_y, LANES), F32),
            pltpu.VMEM((deep, share_x, packs, block_y, LANES), F32),
            pltpu.SemaphoreType.DMA((7 + packs,)),
            pltpu.SemaphoreType.DMA((len(chunks) * packs, north - 1)),
            pltpu.SemaphoreType.DMA((len(chunks) * packs, north - 1)),
            pltpu.SemaphoreType.DMA((len(chunks) * packs, deep)),
            pltpu.SemaphoreType.DMA((len(chunks) * packs, deep)),
        ],
        compiler_params=pltpu.CompilerParams(
            collective_id=0, has_side_effects=True, vmem_limit_bytes=need
        ),
    )(*[pltpu.with_memory_space_constraint(v, pltpu.HBM) for v in operands])


def solution(mesh):
    placed = (P(None, None, "north", "deep"), P(), P(), P(), P())
    return jax.shard_map(
        functools.partial(on_device, mesh.shape["north"], mesh.shape["deep"]),
        mesh=mesh,
        in_specs=placed,
        out_specs=P(None, "north", "deep", None),
        check_vma=False,
    )
```
